32 devices in a mesh: gx: 8 (over y, x, core), gy: 4 (over z).
Axes of the slice: x: 2, y: 2, z: 4, core: 2. Of those that a mesh axis runs over, the one named last changes fastest.
Arguments:
- right_side: float32 [128, 256, 192], P('gx', 'gy'), may hold values from -46 to 46
- diagonal: float32 [128, 256, 192], P('gx', 'gy'), may hold values from 0.1 to 2
Outputs:
- solution_field: float32 [128, 256, 192], P('gx', 'gy')
- residual: float32 [128, 256, 192], P('gx', 'gy')
The draws below stay inside these ranges and needn't reach their ends.
All inputs are finite; a program needn't handle non-finite values.
Results may differ from the reference program's by a relative error of at most 0.00017.
Values sent between devices are 32-bit elements; how exact they have to be, the bound alone decides.
A program may use at most 64 MiB of HBM per device.

```python
import math
import jax
import jax.numpy as jnp

CZ = 192
ITERS = 3
NX = 128
NY = 256


def draw_right_side(key, part):
    first = jax.random.fold_in(key, 11)
    second = jax.random.fold_in(key, 12)
    ramp = 1.0 + 2.0 * jnp.arange(NX, dtype=jnp.float32) / max(NX - 1, 1)
    ramp = ramp.reshape(NX, 1, 1)
    base = jnp.clip(jax.random.normal(first, (NX, NY, CZ), jnp.float32), -5.0, 5.0)
    column = jnp.exp(jax.random.uniform(second, (NX, NY, 1), jnp.float32) * math.log(3.0))
    return ramp * column * base


def levels(rng, extent, split, least, high):
    gain = 1.0
    for position, parts in split:
        draws = jax.random.uniform(jax.random.fold_in(jax.random.fold_in(rng, 6), position), (parts,), jnp.float32, least / len(split), high / len(split))
        gain = gain * jnp.repeat(jnp.exp(draws), extent[position] // parts).reshape((-1,) + (1,) * (len(extent) - 1 - position))
    return gain


def setup_inputs(seed: int = 0) -> dict:
    arg_keys = jax.random.split(jax.random.key(seed), 3)
    return {
        "right_side": draw_right_side(jax.random.fold_in(arg_keys[2], 71), 0),
        "diagonal": jnp.clip(jnp.exp(math.log(2.0) - 2.9957323 * jax.random.uniform(arg_keys[1], (NX, NY, CZ), jnp.float32) ** levels(arg_keys[1], (NX, NY, CZ), ((0, 8), (1, 4)), -0.2, 0.2)), 0.1, 2.0),
    }


def operate(field, diagonal):
    padded = jnp.pad(field, 1)
    beside = padded[2:, 1:-1, 1:-1] + padded[:-2, 1:-1, 1:-1]
    beside = beside + padded[1:-1, 2:, 1:-1] + padded[1:-1, :-2, 1:-1]
    beside = beside + padded[1:-1, 1:-1, 2:] + padded[1:-1, 1:-1, :-2]
    return (6.0 + diagonal) * field - beside


def reference(right_side, diagonal):
    solution_field = jnp.zeros_like(right_side)
    residual = right_side
    w_field = operate(right_side, diagonal)
    z_field = jnp.zeros_like(right_side)
    s_field = jnp.zeros_like(right_side)
    p_field = jnp.zeros_like(right_side)
    gamma_prev = jnp.float32(1.0)
    alpha_prev = jnp.float32(1.0)
    for step in range(ITERS):
        gamma = jnp.sum(residual * residual)
        delta = jnp.sum(w_field * residual)
        if step == 0:
            beta = jnp.float32(0.0)
            alpha = gamma / delta
        else:
            beta = gamma / gamma_prev
            alpha = gamma / (delta - beta * gamma / alpha_prev)
        s_field = w_field + beta * s_field
        p_field = residual + beta * p_field
        solution_field = solution_field + alpha * p_field
        residual = residual - alpha * s_field
        if step + 1 < ITERS:
            q_field = operate(w_field, diagonal)
            z_field = q_field + beta * z_field
            w_field = w_field - alpha * z_field
        gamma_prev = gamma
        alpha_prev = alpha
    return solution_field, residual
```

```python
import functools

import jax
import jax.numpy as jnp
from jax import lax
from jax.experimental import pallas as pl
from jax.experimental.pallas import tpu as pltpu
from jax.sharding import PartitionSpec as P

ITERS = 3
SHIFT = 7.0
MESH = pl.DeviceIdType.MESH
DIRS = ((1, 0), (-1, 0), (0, 1), (0, -1), (1, 1), (1, -1), (-1, 1), (-1, -1))
RIM = ITERS
ROWS = 8


def span_x(step, width, size):
    if step == 0:
        return pl.ds(0, size), pl.ds(RIM, size)
    if step > 0:
        return pl.ds(size - width, width), pl.ds(RIM - width, width)
    return pl.ds(0, width), pl.ds(RIM + size, width)


def span_y(step, size):
    if step == 0:
        return pl.ds(0, size), pl.ds(ROWS, size)
    if step > 0:
        return pl.ds(size - ROWS, ROWS), pl.ds(0, ROWS)
    return pl.ds(0, ROWS), pl.ds(ROWS + size, ROWS)


def times_b(field, shift, layer, valid):
    here = field[layer]
    rows, lanes = here.shape
    row0 = jnp.zeros((1, lanes), jnp.float32)
    lane0 = jnp.zeros((rows, 1), jnp.float32)
    beside = field[layer - 1] + field[layer + 1]
    beside = beside + jnp.concatenate([here[1:], row0], 0)
    beside = beside + jnp.concatenate([row0, here[:-1]], 0)
    beside = beside + jnp.concatenate([here[:, 1:], lane0], 1)
    beside = beside + jnp.concatenate([lane0, here[:, :-1]], 1)
    out = (shift[layer] + (6.0 - SHIFT)) * here - beside
    if valid is None:
        return out
    return jnp.where(valid, out, 0.0)


def coefficients(moments):
    def inner(f, g):
        total = None
        for i, a in enumerate(f):
            for j, c in enumerate(g):
                term = a * c * moments[i + j]
                total = term if total is None else total + term
        return total

    def times_a(f):
        out = [SHIFT * f[0]]
        for k in range(1, len(f)):
            out.append(SHIFT * f[k] + f[k - 1])
        return out + [f[-1]]

    def axpy(f, a, g):
        size = max(len(f), len(g))
        out = []
        for k in range(size):
            if k >= len(f):
                out.append(a * g[k])
            elif k >= len(g):
                out.append(f[k])
            else:
                out.append(f[k] + a * g[k])
        return out

    one = jnp.ones_like(moments[0])
    residual, solution_field = [one], []
    s_field, p_field = [], []
    for step in range(ITERS):
        w_field = times_a(residual)
        gamma = inner(residual, residual)
        delta = inner(w_field, residual)
        if step == 0:
            alpha = gamma / delta
            s_field, p_field = w_field, residual
        else:
            beta = gamma / gamma_prev
            alpha = gamma / (delta - beta * gamma / alpha_prev)
            s_field = axpy(w_field, beta, s_field)
            p_field = axpy(residual, beta, p_field)
        solution_field = axpy(solution_field, alpha, p_field)
        residual = axpy(residual, -alpha, s_field)
        gamma_prev, alpha_prev = gamma, alpha
    return solution_field + residual


def kernel(nx, ny, b_ref, d_ref, v1_ref, v2_ref, v3_ref, co_ref,
           v0, dd, v1, v2, part, planes, middle, lines,
           own_sem, send_sem, recv_sem, px_send, px_recv, py_send, py_recv):
    gx, gy = lax.axis_index("gx"), lax.axis_index("gy")
    bx, by, bz = b_ref.shape
    barrier = pltpu.get_barrier_semaphore()

    def there(dx, dy):
        ok = None
        for at, step, count in ((gx, dx, nx), (gy, dy, ny)):
            if step:
                this = (at + step >= 0) & (at + step < count)
                ok = this if ok is None else ok & this
        return ok

    def peer_x(k):
        return lax.rem(gx + k, nx)

    def peer_y(k):
        return lax.rem(gy + k, ny)

    for dx, dy in DIRS[4:]:
        @pl.when(there(dx, dy))
        def _(dx=dx, dy=dy):
            pl.semaphore_signal(barrier, inc=1, device_id=(gx + dx, gy + dy), device_id_type=MESH)

    @pl.loop(1, nx)
    def _(k):
        pl.semaphore_signal(barrier, inc=1, device_id=(peer_x(k), gy), device_id_type=MESH)

    @pl.loop(1, ny)
    def _(k):
        pl.semaphore_signal(barrier, inc=1, device_id=(gx, peer_y(k)), device_id_type=MESH)

    own = []
    for n, (src, dst) in enumerate(((b_ref, v0), (d_ref, dd))):
        own.append(pltpu.make_async_copy(
            src, dst.at[pl.ds(RIM, bx), pl.ds(ROWS, by), :], own_sem.at[n]))
        own[-1].start()

    @pl.when(gx == 0)
    def _():
        v0[0:RIM] = jnp.zeros((RIM,) + v0.shape[1:], jnp.float32)

    @pl.when(gx == nx - 1)
    def _():
        v0[RIM + bx:] = jnp.zeros((RIM,) + v0.shape[1:], jnp.float32)

    @pl.when(gy == 0)
    def _():
        v0[:, 0:ROWS] = jnp.zeros((v0.shape[0], ROWS, bz), jnp.float32)

    @pl.when(gy == ny - 1)
    def _():
        v0[:, ROWS + by:] = jnp.zeros((v0.shape[0], ROWS, bz), jnp.float32)

    expected = nx - 1 + ny - 1
    for dx, dy in DIRS[4:]:
        expected = expected + there(dx, dy).astype(jnp.int32)
    pl.semaphore_wait(barrier, expected)

    def halo(n, dx, dy):
        width = (RIM, RIM - 1)[n] if dy == 0 else (RIM - 1, RIM - 2)[n]
        src, dst = ((b_ref, v0), (d_ref, dd))[n]
        from_x, to_x = span_x(dx, width, bx)
        from_y, to_y = span_y(dy, by)
        index = DIRS.index((dx, dy))
        return pltpu.make_async_remote_copy(
            src_ref=src.at[from_x, from_y, :],
            dst_ref=dst.at[to_x, to_y, :],
            send_sem=send_sem.at[n, index],
            recv_sem=recv_sem.at[n, index],
            device_id=(gx + dx, gy + dy),
            device_id_type=MESH,
        )

    for n in range(2):
        for dx, dy in DIRS:
            @pl.when(there(dx, dy))
            def _(n=n, dx=dx, dy=dy):
                halo(n, dx, dy).start()

    for copy in own:
        copy.wait()
    for n in range(2):
        for dx, dy in DIRS:
            @pl.when(there(-dx, -dy))
            def _(n=n, dx=dx, dy=dy):
                halo(n, dx, dy).wait_recv()

    row = lax.broadcasted_iota(jnp.int32, (by + 2 * ROWS, bz), 0)
    inside_y = ((row >= ROWS) | (gy > 0)) & ((row < ROWS + by) | (gy < ny - 1))

    def inside(layer):
        ok = ((layer >= RIM) | (gx > 0)) & ((layer < RIM + bx) | (gx < nx - 1))
        return inside_y & ok

    inner = slice(ROWS, ROWS + by)

    @pl.loop(1, 2 * RIM + bx - 1)
    def _(layer):
        v1[layer] = times_b(v0, dd, layer, inside(layer))

    @pl.loop(2, 2 * RIM + bx - 2)
    def _(layer):
        v2[layer] = times_b(v1, dd, layer, inside(layer))

    def tile(a):
        whole = jnp.sum(a.reshape(by // 8, 8, bz), 0)
        pad = jnp.concatenate([whole[:, 128:], jnp.zeros((8, 256 - bz), jnp.float32)], 1)
        return whole[:, :128] + pad

    def body(k, sums):
        layer = k + RIM
        f0 = v0[layer, inner]
        f1 = v1[layer, inner]
        f2 = v2[layer, inner]
        f3 = times_b(v2, dd, layer, None)[inner]
        v1_ref[k] = f1
        v2_ref[k] = f2
        v3_ref[k] = f3
        pairs = (f0 * f0, f0 * f1, f1 * f1, f1 * f2, f2 * f2, f2 * f3)
        return tuple(s + jnp.sum(p.reshape(by // 8, 8, bz), 0) for s, p in zip(sums, pairs))

    sums = lax.fori_loop(0, bx, body, (jnp.zeros((8, bz), jnp.float32),) * 6)
    lane = [jnp.sum(jnp.sum(s, 1, keepdims=True), 0, keepdims=True) for s in sums]
    row8 = lax.broadcasted_iota(jnp.int32, (8, 128), 0)
    packed = jnp.zeros((8, 128), jnp.float32)
    for k, s in enumerate(lane):
        packed = jnp.where(row8 == k, s, packed)
    part[...] = packed

    def share(src, slots, k, axis):
        if axis == 0:
            mine, target = gx, (peer_x(k), gy)
            theirs, sems = lax.rem(gx + nx - k, nx), (px_send, px_recv)
        else:
            mine, target = gy, (gx, peer_y(k))
            theirs, sems = lax.rem(gy + ny - k, ny), (py_send, py_recv)
        return pltpu.make_async_remote_copy(
            src_ref=src, dst_ref=slots.at[mine], send_sem=sems[0].at[k - 1],
            recv_sem=sems[1].at[k - 1], device_id=target, device_id_type=MESH)

    def all_sum(src, slots, count, axis):
        mine = gx if axis == 0 else gy

        @pl.loop(1, count)
        def _(k):
            share(src, slots, k, axis).start()

        slots[mine] = src[...]

        @pl.loop(1, count)
        def _(k):
            share(src, slots, k, axis).wait()

        return lax.fori_loop(1, count, lambda k, t: t + slots[k], slots[0])

    middle[...] = all_sum(part, planes, nx, 0)
    total = all_sum(middle, lines, ny, 1)
    moments = [total[k:k + 1] for k in range(6)]
    co = jnp.zeros((8, 128), jnp.float32)
    for k, c in enumerate(coefficients(moments)):
        co = jnp.where(row8 == k, c, co)
    co_ref[...] = co

    for n in range(2):
        for dx, dy in DIRS:
            @pl.when(there(dx, dy))
            def _(n=n, dx=dx, dy=dy):
                halo(n, dx, dy).wait_send()


def on_device(nx, ny, right_side, diagonal):
    bx, by, bz = right_side.shape
    block = jax.ShapeDtypeStruct((bx, by, bz), jnp.float32)
    big = pltpu.VMEM((bx + 2 * RIM, by + 2 * ROWS, bz), jnp.float32)
    vmem = pl.BlockSpec(memory_space=pltpu.VMEM)
    dma = pltpu.SemaphoreType.DMA
    f1, f2, f3, co = pl.pallas_call(
        functools.partial(kernel, nx, ny),
        out_shape=(block, block, block, jax.ShapeDtypeStruct((8, 128), jnp.float32)),
        in_specs=[pl.BlockSpec(memory_space=pl.ANY)] * 2,
        out_specs=(vmem,) * 4,
        scratch_shapes=[
            big, big, big, big,
            pltpu.VMEM((8, 128), jnp.float32),
            pltpu.VMEM((nx, 8, 128), jnp.float32),
            pltpu.VMEM((8, 128), jnp.float32),
            pltpu.VMEM((ny, 8, 128), jnp.float32),
            dma((2,)), dma((2, 8)), dma((2, 8)),
            dma((nx - 1,)), dma((nx - 1,)), dma((ny - 1,)), dma((ny - 1,)),
        ],
        compiler_params=pltpu.CompilerParams(collective_id=0, has_side_effects=True),
    )(right_side, diagonal)
    c = [co[k, 0] for k in range(7)]
    solution_field = c[0] * right_side + c[1] * f1 + c[2] * f2
    residual = c[3] * right_side + c[4] * f1 + c[5] * f2 + c[6] * f3
    return solution_field, residual


def solution(mesh):
    placed = (P("gx", "gy", None), P("gx", "gy", None))
    return jax.shard_map(
        functools.partial(on_device, mesh.shape["gx"], mesh.shape["gy"]),
        mesh=mesh,
        in_specs=placed,
        out_specs=placed,
        check_vma=False,
    )
```

```python
import functools

import jax
import jax.numpy as jnp
from jax import lax
from jax.experimental import pallas as pl
from jax.experimental.pallas import tpu as pltpu
from jax.sharding import PartitionSpec as P

ITERS = 3
SHIFT = 7.0
MESH = pl.DeviceIdType.MESH
DIRS = ((1, 0), (-1, 0), (0, 1), (0, -1), (1, 1), (1, -1), (-1, 1), (-1, -1))
RIM = ITERS
ROWS = 8


def span_x(step, width, size):
    if step == 0:
        return pl.ds(0, size), pl.ds(RIM, size)
    if step > 0:
        return pl.ds(size - width, width), pl.ds(RIM - width, width)
    return pl.ds(0, width), pl.ds(RIM + size, width)


def span_y(step, width, size):
    if step == 0:
        return pl.ds(0, size), pl.ds(ROWS, size)
    if step > 0:
        return pl.ds(size - width, width), pl.ds(ROWS - width, width)
    return pl.ds(0, width), pl.ds(ROWS + size, width)


def times_b(field, shift, layer, valid):
    here = field[layer]
    rows, lanes = here.shape
    row0 = jnp.zeros((1, lanes), jnp.float32)
    lane0 = jnp.zeros((rows, 1), jnp.float32)
    beside = field[layer - 1] + field[layer + 1]
    beside = beside + jnp.concatenate([here[1:], row0], 0)
    beside = beside + jnp.concatenate([row0, here[:-1]], 0)
    beside = beside + jnp.concatenate([here[:, 1:], lane0], 1)
    beside = beside + jnp.concatenate([lane0, here[:, :-1]], 1)
    out = (shift[layer] + (6.0 - SHIFT)) * here - beside
    if valid is None:
        return out
    return jnp.where(valid, out, 0.0)


def coefficients(moments):
    def inner(f, g):
        total = None
        for i, a in enumerate(f):
            for j, c in enumerate(g):
                term = a * c * moments[i + j]
                total = term if total is None else total + term
        return total

    def times_a(f):
        out = [SHIFT * f[0]]
        for k in range(1, len(f)):
            out.append(SHIFT * f[k] + f[k - 1])
        return out + [f[-1]]

    def axpy(f, a, g):
        size = max(len(f), len(g))
        out = []
        for k in range(size):
            if k >= len(f):
                out.append(a * g[k])
            elif k >= len(g):
                out.append(f[k])
            else:
                out.append(f[k] + a * g[k])
        return out

    one = jnp.ones_like(moments[0])
    residual, solution_field = [one], []
    s_field, p_field = [], []
    for step in range(ITERS):
        w_field = times_a(residual)
        gamma = inner(residual, residual)
        delta = inner(w_field, residual)
        if step == 0:
            alpha = gamma / delta
            s_field, p_field = w_field, residual
        else:
            beta = gamma / gamma_prev
            alpha = gamma / (delta - beta * gamma / alpha_prev)
            s_field = axpy(w_field, beta, s_field)
            p_field = axpy(residual, beta, p_field)
        solution_field = axpy(solution_field, alpha, p_field)
        residual = axpy(residual, -alpha, s_field)
        gamma_prev, alpha_prev = gamma, alpha
    return solution_field + residual


def kernel(nx, ny, b_ref, d_ref, v1_ref, v2_ref, v3_ref, co_ref,
           v0, dd, v1, v2, part, planes, middle, lines,
           own_sem, send_sem, recv_sem, px_send, px_recv, py_send, py_recv):
    gx, gy = lax.axis_index("gx"), lax.axis_index("gy")
    bx, by, bz = b_ref.shape
    barrier = pltpu.get_barrier_semaphore()

    def there(dx, dy):
        ok = None
        for at, step, count in ((gx, dx, nx), (gy, dy, ny)):
            if step:
                this = (at + step >= 0) & (at + step < count)
                ok = this if ok is None else ok & this
        return ok

    def peer_x(k):
        return lax.rem(gx + k, nx)

    def peer_y(k):
        return lax.rem(gy + k, ny)

    for dx, dy in DIRS[4:]:
        @pl.when(there(dx, dy))
        def _(dx=dx, dy=dy):
            pl.semaphore_signal(barrier, inc=1, device_id=(gx + dx, gy + dy), device_id_type=MESH)

    @pl.loop(1, nx)
    def _(k):
        pl.semaphore_signal(barrier, inc=1, device_id=(peer_x(k), gy), device_id_type=MESH)

    @pl.loop(1, ny)
    def _(k):
        pl.semaphore_signal(barrier, inc=1, device_id=(gx, peer_y(k)), device_id_type=MESH)

    own = []
    for n, (src, dst) in enumerate(((b_ref, v0), (d_ref, dd))):
        own.append(pltpu.make_async_copy(
            src, dst.at[pl.ds(RIM, bx), pl.ds(ROWS, by), :], own_sem.at[n]))
        own[-1].start()

    @pl.when(gx == 0)
    def _():
        v0[0:RIM] = jnp.zeros((RIM,) + v0.shape[1:], jnp.float32)

    @pl.when(gx == nx - 1)
    def _():
        v0[RIM + bx:] = jnp.zeros((RIM,) + v0.shape[1:], jnp.float32)

    @pl.when(gy == 0)
    def _():
        v0[:, 0:ROWS] = jnp.zeros((v0.shape[0], ROWS, bz), jnp.float32)

    @pl.when(gy == ny - 1)
    def _():
        v0[:, ROWS + by:] = jnp.zeros((v0.shape[0], ROWS, bz), jnp.float32)

    expected = nx - 1 + ny - 1
    for dx, dy in DIRS[4:]:
        expected = expected + there(dx, dy).astype(jnp.int32)
    pl.semaphore_wait(barrier, expected)

    def halo(n, dx, dy):
        width = RIM - n if dx == 0 or dy == 0 else RIM - 1 - n
        width_y = width
        src, dst = ((b_ref, v0), (d_ref, dd))[n]
        from_x, to_x = span_x(dx, width, bx)
        from_y, to_y = span_y(dy, width_y, by)
        index = DIRS.index((dx, dy))
        return pltpu.make_async_remote_copy(
            src_ref=src.at[from_x, from_y, :],
            dst_ref=dst.at[to_x, to_y, :],
            send_sem=send_sem.at[n, index],
            recv_sem=recv_sem.at[n, index],
            device_id=(gx + dx, gy + dy),
            device_id_type=MESH,
        )

    for n in range(2):
        for dx, dy in DIRS:
            @pl.when(there(dx, dy))
            def _(n=n, dx=dx, dy=dy):
                halo(n, dx, dy).start()

    for copy in own:
        copy.wait()
    for n in range(2):
        for dx, dy in DIRS:
            @pl.when(there(-dx, -dy))
            def _(n=n, dx=dx, dy=dy):
                halo(n, dx, dy).wait_recv()

    row = lax.broadcasted_iota(jnp.int32, (by + 2 * ROWS, bz), 0)
    inside_y = ((row >= ROWS) | (gy > 0)) & ((row < ROWS + by) | (gy < ny - 1))

    def inside(layer):
        ok = ((layer >= RIM) | (gx > 0)) & ((layer < RIM + bx) | (gx < nx - 1))
        return inside_y & ok

    inner = slice(ROWS, ROWS + by)

    @pl.loop(1, 2 * RIM + bx - 1)
    def _(layer):
        v1[layer] = times_b(v0, dd, layer, inside(layer))

    @pl.loop(2, 2 * RIM + bx - 2)
    def _(layer):
        v2[layer] = times_b(v1, dd, layer, inside(layer))

    def tile(a):
        whole = jnp.sum(a.reshape(by // 8, 8, bz), 0)
        pad = jnp.concatenate([whole[:, 128:], jnp.zeros((8, 256 - bz), jnp.float32)], 1)
        return whole[:, :128] + pad

    def body(k, sums):
        layer = k + RIM
        f0 = v0[layer, inner]
        f1 = v1[layer, inner]
        f2 = v2[layer, inner]
        f3 = times_b(v2, dd, layer, None)[inner]
        v1_ref[k] = f1
        v2_ref[k] = f2
        v3_ref[k] = f3
        pairs = (f0 * f0, f0 * f1, f1 * f1, f1 * f2, f2 * f2, f2 * f3)
        return tuple(s + jnp.sum(p.reshape(by // 8, 8, bz), 0) for s, p in zip(sums, pairs))

    sums = lax.fori_loop(0, bx, body, (jnp.zeros((8, bz), jnp.float32),) * 6)
    lane = [jnp.sum(jnp.sum(s, 1, keepdims=True), 0, keepdims=True) for s in sums]
    row8 = lax.broadcasted_iota(jnp.int32, (8, 128), 0)
    packed = jnp.zeros((8, 128), jnp.float32)
    for k, s in enumerate(lane):
        packed = jnp.where(row8 == k, s, packed)
    part[...] = packed

    def share(src, slots, k, axis):
        if axis == 0:
            mine, target = gx, (peer_x(k), gy)
            theirs, sems = lax.rem(gx + nx - k, nx), (px_send, px_recv)
        else:
            mine, target = gy, (gx, peer_y(k))
            theirs, sems = lax.rem(gy + ny - k, ny), (py_send, py_recv)
        return pltpu.make_async_remote_copy(
            src_ref=src, dst_ref=slots.at[mine], send_sem=sems[0].at[k - 1],
            recv_sem=sems[1].at[k - 1], device_id=target, device_id_type=MESH)

    def all_sum(src, slots, count, axis):
        mine = gx if axis == 0 else gy

        @pl.loop(1, count)
        def _(k):
            share(src, slots, k, axis).start()

        slots[mine] = src[...]

        @pl.loop(1, count)
        def _(k):
            share(src, slots, k, axis).wait()

        return lax.fori_loop(1, count, lambda k, t: t + slots[k], slots[0])

    middle[...] = all_sum(part, planes, nx, 0)
    total = all_sum(middle, lines, ny, 1)
    moments = [total[k:k + 1] for k in range(6)]
    co = jnp.zeros((8, 128), jnp.float32)
    for k, c in enumerate(coefficients(moments)):
        co = jnp.where(row8 == k, c, co)
    co_ref[...] = co

    for n in range(2):
        for dx, dy in DIRS:
            @pl.when(there(dx, dy))
            def _(n=n, dx=dx, dy=dy):
                halo(n, dx, dy).wait_send()


def combine(f0_ref, f1_ref, f2_ref, f3_ref, co_ref, x_ref, r_ref, x_out, r_out, sems):
    c = [co_ref[k:k + 1, 0:1] for k in range(7)]
    count = x_out.shape[0]

    def copy(n, k):
        src, dst = ((x_out, x_ref), (r_out, r_ref))[n]
        return pltpu.make_async_copy(src.at[pl.ds(k, 1)], dst.at[pl.ds(k, 1)], sems.at[n, k])

    @pl.loop(0, count)
    def _(k):
        f0, f1, f2, f3 = f0_ref[k], f1_ref[k], f2_ref[k], f3_ref[k]
        x_out[k] = c[0] * f0 + c[1] * f1 + c[2] * f2
        r_out[k] = c[3] * f0 + c[4] * f1 + c[5] * f2 + c[6] * f3
        for n in range(2):
            copy(n, k).start()

    @pl.loop(0, count)
    def _(k):
        for n in range(2):
            copy(n, k).wait()


def on_device(nx, ny, right_side, diagonal):
    bx, by, bz = right_side.shape
    block = jax.ShapeDtypeStruct((bx, by, bz), jnp.float32)
    big = pltpu.VMEM((bx + 2 * RIM, by + 2 * ROWS, bz), jnp.float32)
    vmem = pl.BlockSpec(memory_space=pltpu.VMEM)
    dma = pltpu.SemaphoreType.DMA
    f1, f2, f3, co = pl.pallas_call(
        functools.partial(kernel, nx, ny),
        out_shape=(block, block, block, jax.ShapeDtypeStruct((8, 128), jnp.float32)),
        in_specs=[pl.BlockSpec(memory_space=pltpu.HBM)] * 2,
        out_specs=(vmem,) * 4,
        scratch_shapes=[
            big, big, big, big,
            pltpu.VMEM((8, 128), jnp.float32),
            pltpu.VMEM((nx, 8, 128), jnp.float32),
            pltpu.VMEM((8, 128), jnp.float32),
            pltpu.VMEM((ny, 8, 128), jnp.float32),
            dma((2,)), dma((2, 8)), dma((2, 8)),
            dma((nx - 1,)), dma((nx - 1,)), dma((ny - 1,)), dma((ny - 1,)),
        ],
        compiler_params=pltpu.CompilerParams(
            collective_id=0, has_side_effects=True, vmem_limit_bytes=24 * 2**20),
    )(*(pltpu.with_memory_space_constraint(a, pltpu.HBM) for a in (right_side, diagonal)))
    return pl.pallas_call(
        combine,
        out_shape=(block, block),
        in_specs=[vmem] * 5,
        out_specs=(pl.BlockSpec(memory_space=pl.ANY),) * 2,
        scratch_shapes=[
            pltpu.VMEM((bx, by, bz), jnp.float32),
            pltpu.VMEM((bx, by, bz), jnp.float32),
            dma((2, bx)),
        ],
        compiler_params=pltpu.CompilerParams(vmem_limit_bytes=24 * 2**20),
    )(right_side, f1, f2, f3, co)


def solution(mesh):
    placed = (P("gx", "gy", None), P("gx", "gy", None))
    return jax.shard_map(
        functools.partial(on_device, mesh.shape["gx"], mesh.shape["gy"]),
        mesh=mesh,
        in_specs=placed,
        out_specs=placed,
        check_vma=False,
    )
```

```python
import functools

import jax
import jax.numpy as jnp
from jax import lax
from jax.experimental import pallas as pl
from jax.experimental.pallas import tpu as pltpu
from jax.sharding import PartitionSpec as P

ITERS = 3
SHIFT = 7.0
MESH = pl.DeviceIdType.MESH
DIRS = ((1, 0), (-1, 0), (0, 1), (0, -1), (1, 1), (1, -1), (-1, 1), (-1, -1))
RIM = ITERS
ROWS = 8


def span_x(step, width, size):
    if step == 0:
        return pl.ds(0, size), pl.ds(RIM, size)
    if step > 0:
        return pl.ds(size - width, width), pl.ds(RIM - width, width)
    return pl.ds(0, width), pl.ds(RIM + size, width)


def span_y(step, width, size):
    if step == 0:
        return pl.ds(0, size), pl.ds(ROWS, size)
    if step > 0:
        return pl.ds(size - width, width), pl.ds(ROWS - width, width)
    return pl.ds(0, width), pl.ds(ROWS + size, width)


def times_b(field, shift, layer, valid):
    here = field[layer]
    rows, lanes = here.shape
    row0 = jnp.zeros((1, lanes), jnp.float32)
    lane0 = jnp.zeros((rows, 1), jnp.float32)
    beside = field[layer - 1] + field[layer + 1]
    beside = beside + jnp.concatenate([here[1:], row0], 0)
    beside = beside + jnp.concatenate([row0, here[:-1]], 0)
    beside = beside + jnp.concatenate([here[:, 1:], lane0], 1)
    beside = beside + jnp.concatenate([lane0, here[:, :-1]], 1)
    out = (shift[layer] + (6.0 - SHIFT)) * here - beside
    if valid is None:
        return out
    return jnp.where(valid, out, 0.0)


def coefficients(moments):
    def inner(f, g):
        total = None
        for i, a in enumerate(f):
            for j, c in enumerate(g):
                term = a * c * moments[i + j]
                total = term if total is None else total + term
        return total

    def times_a(f):
        out = [SHIFT * f[0]]
        for k in range(1, len(f)):
            out.append(SHIFT * f[k] + f[k - 1])
        return out + [f[-1]]

    def axpy(f, a, g):
        size = max(len(f), len(g))
        out = []
        for k in range(size):
            if k >= len(f):
                out.append(a * g[k])
            elif k >= len(g):
                out.append(f[k])
            else:
                out.append(f[k] + a * g[k])
        return out

    one = jnp.ones_like(moments[0])
    residual, solution_field = [one], []
    s_field, p_field = [], []
    for step in range(ITERS):
        w_field = times_a(residual)
        gamma = inner(residual, residual)
        delta = inner(w_field, residual)
        if step == 0:
            alpha = gamma / delta
            s_field, p_field = w_field, residual
        else:
            beta = gamma / gamma_prev
            alpha = gamma / (delta - beta * gamma / alpha_prev)
            s_field = axpy(w_field, beta, s_field)
            p_field = axpy(residual, beta, p_field)
        solution_field = axpy(solution_field, alpha, p_field)
        residual = axpy(residual, -alpha, s_field)
        gamma_prev, alpha_prev = gamma, alpha
    return solution_field + residual


def kernel(nx, ny, b_ref, d_ref, v1_ref, v2_ref, v3_ref, co_ref,
           v0, dd, v1, v2, part, planes, middle, lines,
           own_sem, send_sem, recv_sem, px_send, px_recv, py_send, py_recv):
    gx, gy = lax.axis_index("gx"), lax.axis_index("gy")
    bx, by, bz = b_ref.shape
    barrier = pltpu.get_barrier_semaphore()

    def there(dx, dy):
        ok = None
        for at, step, count in ((gx, dx, nx), (gy, dy, ny)):
            if step:
                this = (at + step >= 0) & (at + step < count)
                ok = this if ok is None else ok & this
        return ok

    def peer_x(k):
        return lax.rem(gx + k, nx)

    def peer_y(k):
        return lax.rem(gy + k, ny)

    for dx, dy in DIRS[4:]:
        @pl.when(there(dx, dy))
        def _(dx=dx, dy=dy):
            pl.semaphore_signal(barrier, inc=1, device_id=(gx + dx, gy + dy), device_id_type=MESH)

    @pl.loop(1, nx)
    def _(k):
        pl.semaphore_signal(barrier, inc=1, device_id=(peer_x(k), gy), device_id_type=MESH)

    @pl.loop(1, ny)
    def _(k):
        pl.semaphore_signal(barrier, inc=1, device_id=(gx, peer_y(k)), device_id_type=MESH)

    own = []
    for n, (src, dst) in enumerate(((b_ref, v0), (d_ref, dd))):
        own.append(pltpu.make_async_copy(
            src, dst.at[pl.ds(RIM, bx), pl.ds(ROWS, by), :], own_sem.at[n]))
        own[-1].start()

    @pl.when(gx == 0)
    def _():
        v0[0:RIM] = jnp.zeros((RIM,) + v0.shape[1:], jnp.float32)

    @pl.when(gx == nx - 1)
    def _():
        v0[RIM + bx:] = jnp.zeros((RIM,) + v0.shape[1:], jnp.float32)

    @pl.when(gy == 0)
    def _():
        v0[:, 0:ROWS] = jnp.zeros((v0.shape[0], ROWS, bz), jnp.float32)

    @pl.when(gy == ny - 1)
    def _():
        v0[:, ROWS + by:] = jnp.zeros((v0.shape[0], ROWS, bz), jnp.float32)

    expected = nx - 1 + ny - 1
    for dx, dy in DIRS[4:]:
        expected = expected + there(dx, dy).astype(jnp.int32)
    pl.semaphore_wait(barrier, expected)

    def halo(n, dx, dy):
        width = RIM - n if dx == 0 or dy == 0 else RIM - 1 - n
        width_y = width
        src, dst = ((b_ref, v0), (d_ref, dd))[n]
        from_x, to_x = span_x(dx, width, bx)
        from_y, to_y = span_y(dy, width_y, by)
        index = DIRS.index((dx, dy))
        return pltpu.make_async_remote_copy(
            src_ref=src.at[from_x, from_y, :],
            dst_ref=dst.at[to_x, to_y, :],
            send_sem=send_sem.at[n, index],
            recv_sem=recv_sem.at[n, index],
            device_id=(gx + dx, gy + dy),
            device_id_type=MESH,
        )

    for n in range(2):
        for dx, dy in DIRS:
            @pl.when(there(dx, dy))
            def _(n=n, dx=dx, dy=dy):
                halo(n, dx, dy).start()

    def arrived(directions):
        for n in range(2):
            for dx, dy in directions:
                @pl.when(there(-dx, -dy))
                def _(n=n, dx=dx, dy=dy):
                    halo(n, dx, dy).wait_recv()

    row = lax.broadcasted_iota(jnp.int32, (by + 2 * ROWS, bz), 0)
    inside_y = ((row >= ROWS) | (gy > 0)) & ((row < ROWS + by) | (gy < ny - 1))

    def inside(layer):
        ok = ((layer >= RIM) | (gx > 0)) & ((layer < RIM + bx) | (gx < nx - 1))
        return inside_y & ok

    inner = slice(ROWS, ROWS + by)

    def body(layer, sums):
        k = layer - RIM
        f0 = v0[layer, inner]
        f1 = v1[layer, inner]
        f2 = v2[layer, inner]
        f3 = times_b(v2, dd, layer, None)[inner]
        v1_ref[k] = f1
        v2_ref[k] = f2
        v3_ref[k] = f3
        pairs = (f0 * f0, f0 * f1, f1 * f1, f1 * f2, f2 * f2, f2 * f3)
        return tuple(s + jnp.sum(p.reshape(by // 8, 8, bz), 0) for s, p in zip(sums, pairs))

    def stencils(starts, count, valid, sums):
        @pl.loop(0, count[0])
        def _(k):
            layer = starts[0] + k
            v1[layer] = times_b(v0, dd, layer, valid(layer))

        @pl.loop(0, count[1])
        def _(k):
            layer = starts[1] + k
            v2[layer] = times_b(v1, dd, layer, valid(layer))

        return lax.fori_loop(0, count[2], lambda k, s: body(starts[2] + k, s), sums)

    for copy in own:
        copy.wait()
    arrived(DIRS[2:4])
    sums = (jnp.zeros((8, bz), jnp.float32),) * 6
    sums = stencils((RIM + 1, RIM + 2, RIM + 3), (bx - 2, bx - 4, bx - 6), lambda layer: inside_y, sums)
    near_high = lax.rem(gx, 2) == 0
    for turn in range(2):
        high = near_high if turn == 0 else jnp.logical_not(near_high)

        @pl.when(high)
        def _():
            arrived([d for d in DIRS if d[0] < 0])

        @pl.when(jnp.logical_not(high))
        def _():
            arrived([d for d in DIRS if d[0] > 0])

        starts = tuple(jnp.where(high, RIM + bx - 1 - k, RIM - 2 + k) for k in range(3))
        sums = stencils(starts, (3, 3, 3), inside, sums)

    lane = [jnp.sum(jnp.sum(s, 1, keepdims=True), 0, keepdims=True) for s in sums]
    row8 = lax.broadcasted_iota(jnp.int32, (8, 128), 0)
    packed = jnp.zeros((8, 128), jnp.float32)
    for k, s in enumerate(lane):
        packed = jnp.where(row8 == k, s, packed)
    part[...] = packed

    def share(src, slots, k, axis):
        if axis == 0:
            mine, target = gx, (peer_x(k), gy)
            theirs, sems = lax.rem(gx + nx - k, nx), (px_send, px_recv)
        else:
            mine, target = gy, (gx, peer_y(k))
            theirs, sems = lax.rem(gy + ny - k, ny), (py_send, py_recv)
        return pltpu.make_async_remote_copy(
            src_ref=src, dst_ref=slots.at[mine], send_sem=sems[0].at[k - 1],
            recv_sem=sems[1].at[k - 1], device_id=target, device_id_type=MESH)

    def all_sum(src, slots, count, axis):
        mine = gx if axis == 0 else gy

        @pl.loop(1, count)
        def _(k):
            share(src, slots, k, axis).start()

        slots[mine] = src[...]

        @pl.loop(1, count)
        def _(k):
            share(src, slots, k, axis).wait()

        return lax.fori_loop(1, count, lambda k, t: t + slots[k], slots[0])

    middle[...] = all_sum(part, planes, nx, 0)
    total = all_sum(middle, lines, ny, 1)
    moments = [total[k:k + 1] for k in range(6)]
    co = jnp.zeros((8, 128), jnp.float32)
    for k, c in enumerate(coefficients(moments)):
        co = jnp.where(row8 == k, c, co)
    co_ref[...] = co

    for n in range(2):
        for dx, dy in DIRS:
            @pl.when(there(dx, dy))
            def _(n=n, dx=dx, dy=dy):
                halo(n, dx, dy).wait_send()


def combine(f0_ref, f1_ref, f2_ref, f3_ref, co_ref, x_ref, r_ref, x_out, r_out, sems):
    c = [co_ref[k:k + 1, 0:1] for k in range(7)]
    count = x_out.shape[0]

    def copy(n, k):
        src, dst = ((x_out, x_ref), (r_out, r_ref))[n]
        return pltpu.make_async_copy(src.at[pl.ds(k, 1)], dst.at[pl.ds(k, 1)], sems.at[n, k])

    @pl.loop(0, count)
    def _(k):
        f0, f1, f2, f3 = f0_ref[k], f1_ref[k], f2_ref[k], f3_ref[k]
        x_out[k] = c[0] * f0 + c[1] * f1 + c[2] * f2
        r_out[k] = c[3] * f0 + c[4] * f1 + c[5] * f2 + c[6] * f3
        for n in range(2):
            copy(n, k).start()

    @pl.loop(0, count)
    def _(k):
        for n in range(2):
            copy(n, k).wait()


def on_device(nx, ny, right_side, diagonal):
    bx, by, bz = right_side.shape
    block = jax.ShapeDtypeStruct((bx, by, bz), jnp.float32)
    big = pltpu.VMEM((bx + 2 * RIM, by + 2 * ROWS, bz), jnp.float32)
    vmem = pl.BlockSpec(memory_space=pltpu.VMEM)
    dma = pltpu.SemaphoreType.DMA
    f1, f2, f3, co = pl.pallas_call(
        functools.partial(kernel, nx, ny),
        out_shape=(block, block, block, jax.ShapeDtypeStruct((8, 128), jnp.float32)),
        in_specs=[pl.BlockSpec(memory_space=pltpu.HBM)] * 2,
        out_specs=(vmem,) * 4,
        scratch_shapes=[
            big, big, big, big,
            pltpu.VMEM((8, 128), jnp.float32),
            pltpu.VMEM((nx, 8, 128), jnp.float32),
            pltpu.VMEM((8, 128), jnp.float32),
            pltpu.VMEM((ny, 8, 128), jnp.float32),
            dma((2,)), dma((2, 8)), dma((2, 8)),
            dma((nx - 1,)), dma((nx - 1,)), dma((ny - 1,)), dma((ny - 1,)),
        ],
        compiler_params=pltpu.CompilerParams(
            collective_id=0, has_side_effects=True, vmem_limit_bytes=24 * 2**20),
    )(*(pltpu.with_memory_space_constraint(a, pltpu.HBM) for a in (right_side, diagonal)))
    return pl.pallas_call(
        combine,
        out_shape=(block, block),
        in_specs=[vmem] * 5,
        out_specs=(pl.BlockSpec(memory_space=pl.ANY),) * 2,
        scratch_shapes=[
            pltpu.VMEM((bx, by, bz), jnp.float32),
            pltpu.VMEM((bx, by, bz), jnp.float32),
            dma((2, bx)),
        ],
        compiler_params=pltpu.CompilerParams(vmem_limit_bytes=24 * 2**20),
    )(right_side, f1, f2, f3, co)


def solution(mesh):
    placed = (P("gx", "gy", None), P("gx", "gy", None))
    return jax.shard_map(
        functools.partial(on_device, mesh.shape["gx"], mesh.shape["gy"]),
        mesh=mesh,
        in_specs=placed,
        out_specs=placed,
        check_vma=False,
    )
```

```python
import functools

import jax
import jax.numpy as jnp
from jax import lax
from jax.experimental import pallas as pl
from jax.experimental.pallas import tpu as pltpu
from jax.sharding import PartitionSpec as P

ITERS = 3
SHIFT = 7.0
MESH = pl.DeviceIdType.MESH
DIRS = ((1, 0), (-1, 0), (0, 1), (0, -1), (1, 1), (1, -1), (-1, 1), (-1, -1))
RIM = ITERS
ROWS = 8


def span_x(step, width, size):
    if step == 0:
        return pl.ds(0, size), pl.ds(RIM, size)
    if step > 0:
        return pl.ds(size - width, width), pl.ds(RIM - width, width)
    return pl.ds(0, width), pl.ds(RIM + size, width)


def span_y(step, width, size):
    if step == 0:
        return pl.ds(0, size), pl.ds(ROWS, size)
    if step > 0:
        return pl.ds(size - width, width), pl.ds(ROWS - width, width)
    return pl.ds(0, width), pl.ds(ROWS + size, width)


def times_b(field, shift, layer, valid):
    here = field[layer]
    rows, lanes = here.shape
    row0 = jnp.zeros((1, lanes), jnp.float32)
    lane0 = jnp.zeros((rows, 1), jnp.float32)
    beside = field[layer - 1] + field[layer + 1]
    beside = beside + jnp.concatenate([here[1:], row0], 0)
    beside = beside + jnp.concatenate([row0, here[:-1]], 0)
    beside = beside + jnp.concatenate([here[:, 1:], lane0], 1)
    beside = beside + jnp.concatenate([lane0, here[:, :-1]], 1)
    out = (shift[layer] + (6.0 - SHIFT)) * here - beside
    if valid is None:
        return out
    return jnp.where(valid, out, 0.0)


def coefficients(moments):
    def inner(f, g):
        total = None
        for i, a in enumerate(f):
            for j, c in enumerate(g):
                term = a * c * moments[i + j]
                total = term if total is None else total + term
        return total

    def times_a(f):
        out = [SHIFT * f[0]]
        for k in range(1, len(f)):
            out.append(SHIFT * f[k] + f[k - 1])
        return out + [f[-1]]

    def axpy(f, a, g):
        size = max(len(f), len(g))
        out = []
        for k in range(size):
            if k >= len(f):
                out.append(a * g[k])
            elif k >= len(g):
                out.append(f[k])
            else:
                out.append(f[k] + a * g[k])
        return out

    one = jnp.ones_like(moments[0])
    residual, solution_field = [one], []
    s_field, p_field = [], []
    for step in range(ITERS):
        w_field = times_a(residual)
        gamma = inner(residual, residual)
        delta = inner(w_field, residual)
        if step == 0:
            alpha = gamma / delta
            s_field, p_field = w_field, residual
        else:
            beta = gamma / gamma_prev
            alpha = gamma / (delta - beta * gamma / alpha_prev)
            s_field = axpy(w_field, beta, s_field)
            p_field = axpy(residual, beta, p_field)
        solution_field = axpy(solution_field, alpha, p_field)
        residual = axpy(residual, -alpha, s_field)
        gamma_prev, alpha_prev = gamma, alpha
    return solution_field + residual


def kernel(nx, ny, b_ref, d_ref, v1_ref, v2_ref, v3_ref, co_ref,
           v0, dd, v1, v2, part, slots,
           own_sem, send_sem, recv_sem, sum_send, sum_recv):
    gx, gy = lax.axis_index("gx"), lax.axis_index("gy")
    bx, by, bz = b_ref.shape
    barrier = pltpu.get_barrier_semaphore()

    def there(dx, dy):
        ok = None
        for at, step, count in ((gx, dx, nx), (gy, dy, ny)):
            if step:
                this = (at + step >= 0) & (at + step < count)
                ok = this if ok is None else ok & this
        return ok

    def peer_x(k):
        return lax.rem(gx + k, nx)

    def peer_y(k):
        return lax.rem(gy + k, ny)

    count = nx * ny
    me = gx * ny + gy

    def peer(k):
        to = lax.rem(me + k, count)
        return to // ny, lax.rem(to, ny)

    @pl.loop(1, count)
    def _(k):
        pl.semaphore_signal(barrier, inc=1, device_id=peer(k), device_id_type=MESH)

    own = []
    for n, (src, dst) in enumerate(((b_ref, v0), (d_ref, dd))):
        own.append(pltpu.make_async_copy(
            src, dst.at[pl.ds(RIM, bx), pl.ds(ROWS, by), :], own_sem.at[n]))
        own[-1].start()

    @pl.when(gx == 0)
    def _():
        v0[0:RIM] = jnp.zeros((RIM,) + v0.shape[1:], jnp.float32)

    @pl.when(gx == nx - 1)
    def _():
        v0[RIM + bx:] = jnp.zeros((RIM,) + v0.shape[1:], jnp.float32)

    @pl.when(gy == 0)
    def _():
        v0[:, 0:ROWS] = jnp.zeros((v0.shape[0], ROWS, bz), jnp.float32)

    @pl.when(gy == ny - 1)
    def _():
        v0[:, ROWS + by:] = jnp.zeros((v0.shape[0], ROWS, bz), jnp.float32)

    pl.semaphore_wait(barrier, count - 1)

    def halo(n, dx, dy):
        width = RIM - n if dx == 0 or dy == 0 else RIM - 1 - n
        width_y = width
        dst = (v0, dd)[n]
        src = dst.at[pl.ds(RIM, bx), pl.ds(ROWS, by), :]
        from_x, to_x = span_x(dx, width, bx)
        from_y, to_y = span_y(dy, width_y, by)
        index = DIRS.index((dx, dy))
        return pltpu.make_async_remote_copy(
            src_ref=src.at[from_x, from_y, :],
            dst_ref=dst.at[to_x, to_y, :],
            send_sem=send_sem.at[n, index],
            recv_sem=recv_sem.at[n, index],
            device_id=(gx + dx, gy + dy),
            device_id_type=MESH,
        )

    for copy in own:
        copy.wait()
    for n in range(2):
        for dx, dy in DIRS:
            @pl.when(there(dx, dy))
            def _(n=n, dx=dx, dy=dy):
                halo(n, dx, dy).start()

    def arrived(directions):
        for n in range(2):
            for dx, dy in directions:
                @pl.when(there(-dx, -dy))
                def _(n=n, dx=dx, dy=dy):
                    halo(n, dx, dy).wait_recv()

    row = lax.broadcasted_iota(jnp.int32, (by + 2 * ROWS, bz), 0)
    inside_y = ((row >= ROWS) | (gy > 0)) & ((row < ROWS + by) | (gy < ny - 1))

    def inside(layer):
        ok = ((layer >= RIM) | (gx > 0)) & ((layer < RIM + bx) | (gx < nx - 1))
        return inside_y & ok

    inner = slice(ROWS, ROWS + by)

    def body(layer, sums):
        k = layer - RIM
        f0 = v0[layer, inner]
        f1 = v1[layer, inner]
        f2 = v2[layer, inner]
        f3 = times_b(v2, dd, layer, None)[inner]
        v1_ref[k] = f1
        v2_ref[k] = f2
        v3_ref[k] = f3
        pairs = (f0 * f0, f0 * f1, f1 * f1, f1 * f2, f2 * f2, f2 * f3)
        return tuple(s + jnp.sum(p.reshape(by // 8, 8, bz), 0) for s, p in zip(sums, pairs))

    def stencils(starts, count, valid, sums):
        @pl.loop(0, count[0])
        def _(k):
            layer = starts[0] + k
            v1[layer] = times_b(v0, dd, layer, valid(layer))

        @pl.loop(0, count[1])
        def _(k):
            layer = starts[1] + k
            v2[layer] = times_b(v1, dd, layer, valid(layer))

        return lax.fori_loop(0, count[2], lambda k, s: body(starts[2] + k, s), sums)

    arrived(DIRS[2:4])
    sums = (jnp.zeros((8, bz), jnp.float32),) * 6
    sums = stencils((RIM + 1, RIM + 2, RIM + 3), (bx - 2, bx - 4, bx - 6), lambda layer: inside_y, sums)
    near_high = lax.rem(gx, 2) == 0
    for turn in range(2):
        high = near_high if turn == 0 else jnp.logical_not(near_high)

        @pl.when(high)
        def _():
            arrived([d for d in DIRS if d[0] < 0])

        @pl.when(jnp.logical_not(high))
        def _():
            arrived([d for d in DIRS if d[0] > 0])

        starts = tuple(jnp.where(high, RIM + bx - 1 - k, RIM - 2 + k) for k in range(3))
        sums = stencils(starts, (3, 3, 3), inside, sums)

    lane = [jnp.sum(jnp.sum(s, 1, keepdims=True), 0, keepdims=True) for s in sums]
    lane_of = lax.broadcasted_iota(jnp.int32, (1, 128), 1)
    packed = jnp.zeros((1, 128), jnp.float32)
    for k, s in enumerate(lane):
        packed = jnp.where(lane_of == k, s, packed)
    part[0] = packed

    @pl.loop(1, count)
    def _(k):
        pltpu.make_async_remote_copy(
            src_ref=part.at[0], dst_ref=slots.at[me], send_sem=sum_send.at[0],
            recv_sem=sum_recv.at[0], device_id=peer(k), device_id_type=MESH).start()

    slots[me] = packed
    others = slots.at[pl.ds(0, count - 1)]
    pltpu.make_async_copy(others, others, sum_recv.at[0]).wait()
    total = jnp.sum(slots[...], 0)
    moments = [total[:, k:k + 1] for k in range(6)]
    row8 = lax.broadcasted_iota(jnp.int32, (8, 128), 0)
    co = jnp.zeros((8, 128), jnp.float32)
    for k, c in enumerate(coefficients(moments)):
        co = jnp.where(row8 == k, c, co)
    co_ref[...] = co
    pltpu.make_async_copy(others, others, sum_send.at[0]).wait()

    for n in range(2):
        for dx, dy in DIRS:
            @pl.when(there(dx, dy))
            def _(n=n, dx=dx, dy=dy):
                halo(n, dx, dy).wait_send()


def combine(f0_ref, f1_ref, f2_ref, f3_ref, co_ref, x_ref, r_ref, x_out, r_out, sems):
    c = [co_ref[k:k + 1, 0:1] for k in range(7)]
    count = x_out.shape[0]

    def copy(n, k):
        src, dst = ((x_out, x_ref), (r_out, r_ref))[n]
        return pltpu.make_async_copy(src.at[pl.ds(k, 1)], dst.at[pl.ds(k, 1)], sems.at[n, k])

    @pl.loop(0, count)
    def _(k):
        f0, f1, f2, f3 = f0_ref[k], f1_ref[k], f2_ref[k], f3_ref[k]
        x_out[k] = c[0] * f0 + c[1] * f1 + c[2] * f2
        r_out[k] = c[3] * f0 + c[4] * f1 + c[5] * f2 + c[6] * f3
        for n in range(2):
            copy(n, k).start()

    @pl.loop(0, count)
    def _(k):
        for n in range(2):
            copy(n, k).wait()


def on_device(nx, ny, right_side, diagonal):
    bx, by, bz = right_side.shape
    block = jax.ShapeDtypeStruct((bx, by, bz), jnp.float32)
    big = pltpu.VMEM((bx + 2 * RIM, by + 2 * ROWS, bz), jnp.float32)
    vmem = pl.BlockSpec(memory_space=pltpu.VMEM)
    dma = pltpu.SemaphoreType.DMA
    f1, f2, f3, co = pl.pallas_call(
        functools.partial(kernel, nx, ny),
        out_shape=(block, block, block, jax.ShapeDtypeStruct((8, 128), jnp.float32)),
        in_specs=[pl.BlockSpec(memory_space=pltpu.HBM)] * 2,
        out_specs=(vmem,) * 4,
        scratch_shapes=[
            big, big, big, big,
            pltpu.VMEM((1, 1, 128), jnp.float32),
            pltpu.VMEM((nx * ny, 1, 128), jnp.float32),
            dma((2,)), dma((2, 8)), dma((2, 8)),
            dma((1,)), dma((1,)),
        ],
        compiler_params=pltpu.CompilerParams(
            collective_id=0, has_side_effects=True, vmem_limit_bytes=24 * 2**20),
    )(*(pltpu.with_memory_space_constraint(a, pltpu.HBM) for a in (right_side, diagonal)))
    return pl.pallas_call(
        combine,
        out_shape=(block, block),
        in_specs=[vmem] * 5,
        out_specs=(pl.BlockSpec(memory_space=pl.ANY),) * 2,
        scratch_shapes=[
            pltpu.VMEM((bx, by, bz), jnp.float32),
            pltpu.VMEM((bx, by, bz), jnp.float32),
            dma((2, bx)),
        ],
        compiler_params=pltpu.CompilerParams(vmem_limit_bytes=24 * 2**20),
    )(right_side, f1, f2, f3, co)


def solution(mesh):
    placed = (P("gx", "gy", None), P("gx", "gy", None))
    return jax.shard_map(
        functools.partial(on_device, mesh.shape["gx"], mesh.shape["gy"]),
        mesh=mesh,
        in_specs=placed,
        out_specs=placed,
        check_vma=False,
    )
```

```python
import functools

import jax
import jax.numpy as jnp
from jax import lax
from jax.experimental import pallas as pl
from jax.experimental.pallas import tpu as pltpu
from jax.sharding import PartitionSpec as P

ITERS = 3
SHIFT = 7.0
MESH = pl.DeviceIdType.MESH
DIRS = ((1, 0), (-1, 0), (0, 1), (0, -1), (1, 1), (1, -1), (-1, 1), (-1, -1))
RIM = ITERS
ROWS = 8


def span_x(step, width, size):
    if step == 0:
        return pl.ds(0, size), pl.ds(RIM, size)
    if step > 0:
        return pl.ds(size - width, width), pl.ds(RIM - width, width)
    return pl.ds(0, width), pl.ds(RIM + size, width)


def span_y(step, width, size):
    if step == 0:
        return pl.ds(0, size), pl.ds(ROWS, size)
    if step > 0:
        return pl.ds(size - width, width), pl.ds(ROWS - width, width)
    return pl.ds(0, width), pl.ds(ROWS + size, width)


def times_b(field, shift, layer, valid, span=slice(None)):
    here = field[layer, span]
    rows, lanes = here.shape
    row0 = jnp.zeros((1, lanes), jnp.float32)
    lane0 = jnp.zeros((rows, 1), jnp.float32)
    beside = field[layer - 1, span] + field[layer + 1, span]
    beside = beside + jnp.concatenate([here[1:], row0], 0)
    beside = beside + jnp.concatenate([row0, here[:-1]], 0)
    beside = beside + jnp.concatenate([here[:, 1:], lane0], 1)
    beside = beside + jnp.concatenate([lane0, here[:, :-1]], 1)
    out = (shift[layer, span] + (6.0 - SHIFT)) * here - beside
    if valid is None:
        return out
    return jnp.where(valid, out, 0.0)


def coefficients(moments):
    def inner(f, g):
        total = None
        for i, a in enumerate(f):
            for j, c in enumerate(g):
                term = a * c * moments[i + j]
                total = term if total is None else total + term
        return total

    def times_a(f):
        out = [SHIFT * f[0]]
        for k in range(1, len(f)):
            out.append(SHIFT * f[k] + f[k - 1])
        return out + [f[-1]]

    def axpy(f, a, g):
        size = max(len(f), len(g))
        out = []
        for k in range(size):
            if k >= len(f):
                out.append(a * g[k])
            elif k >= len(g):
                out.append(f[k])
            else:
                out.append(f[k] + a * g[k])
        return out

    one = jnp.ones_like(moments[0])
    residual, solution_field = [one], []
    s_field, p_field = [], []
    for step in range(ITERS):
        w_field = times_a(residual)
        gamma = inner(residual, residual)
        delta = inner(w_field, residual)
        if step == 0:
            alpha = gamma / delta
            s_field, p_field = w_field, residual
        else:
            beta = gamma / gamma_prev
            alpha = gamma / (delta - beta * gamma / alpha_prev)
            s_field = axpy(w_field, beta, s_field)
            p_field = axpy(residual, beta, p_field)
        solution_field = axpy(solution_field, alpha, p_field)
        residual = axpy(residual, -alpha, s_field)
        gamma_prev, alpha_prev = gamma, alpha
    return solution_field + residual


def kernel(nx, ny, b_ref, d_ref, v1_ref, v2_ref, v3_ref, co_ref,
           v0, dd, v1, v2, part, slots,
           tail_out, tail_in, own_sem, send_sem, recv_sem, sum_send, sum_recv, tail_send, tail_recv):
    gx, gy = lax.axis_index("gx"), lax.axis_index("gy")
    bx, by, bz = b_ref.shape
    barrier = pltpu.get_barrier_semaphore()

    def there(dx, dy):
        ok = None
        for at, step, count in ((gx, dx, nx), (gy, dy, ny)):
            if step:
                this = (at + step >= 0) & (at + step < count)
                ok = this if ok is None else ok & this
        return ok

    def peer_x(k):
        return lax.rem(gx + k, nx)

    def peer_y(k):
        return lax.rem(gy + k, ny)

    count = nx * ny
    me = gx * ny + gy

    def peer(k):
        to = lax.rem(me + k, count)
        return to // ny, lax.rem(to, ny)

    @pl.loop(1, count)
    def _(k):
        pl.semaphore_signal(barrier, inc=1, device_id=peer(k), device_id_type=MESH)

    own = []
    for n, (src, dst) in enumerate(((b_ref, v0), (d_ref, dd))):
        own.append(pltpu.make_async_copy(
            src, dst.at[pl.ds(RIM, bx), pl.ds(ROWS, by), :], own_sem.at[n]))
        own[-1].start()

    @pl.when(gx == 0)
    def _():
        v0[0:RIM] = jnp.zeros((RIM,) + v0.shape[1:], jnp.float32)

    @pl.when(gx == nx - 1)
    def _():
        v0[RIM + bx:] = jnp.zeros((RIM,) + v0.shape[1:], jnp.float32)

    @pl.when(gy == 0)
    def _():
        v0[:, 0:ROWS] = jnp.zeros((v0.shape[0], ROWS, bz), jnp.float32)

    @pl.when(gy == ny - 1)
    def _():
        v0[:, ROWS + by:] = jnp.zeros((v0.shape[0], ROWS, bz), jnp.float32)

    def halo(n, dx, dy):
        width = RIM - n if dx == 0 or dy == 0 else RIM - 1 - n
        width_y = width
        dst = (v0, dd)[n]
        src = dst.at[pl.ds(RIM, bx), pl.ds(ROWS, by), :]
        from_x, to_x = span_x(dx, width, bx)
        from_y, to_y = span_y(dy, width_y, by)
        index = DIRS.index((dx, dy))
        lanes = pl.ds(0, bz // 128 * 128) if dy == 0 else slice(None)
        return pltpu.make_async_remote_copy(
            src_ref=src.at[from_x, from_y, lanes],
            dst_ref=dst.at[to_x, to_y, lanes],
            send_sem=send_sem.at[n, index],
            recv_sem=recv_sem.at[n, index],
            device_id=(gx + dx, gy + dy),
            device_id_type=MESH,
        )

    for copy in own:
        copy.wait()
    full = bz // 128 * 128
    tail = bz - full
    half = by // 2
    last = pl.ds(full, tail)

    def tails(dx, sending):
        first, second = pl.ds(0, tail), pl.ds(tail, tail)
        low = {(True, 1): RIM + bx - 1, (True, -1): RIM, (False, 1): RIM - 1,
               (False, -1): RIM + bx}[sending, dx]
        at = [low - dx * k for k in range(RIM)]
        every = pl.ds(ROWS, by)
        return (
            (v0, at[0], every, pl.ds(0, by), first),
            (v0, at[1], every, pl.ds(0, by), second),
            (v0, at[2], every, pl.ds(by, by), first),
            (dd, at[0], every, pl.ds(by, by), second),
            (dd, at[1], pl.ds(ROWS, half), pl.ds(2 * by, half), first),
            (dd, at[1], pl.ds(ROWS + half, half), pl.ds(2 * by, half), second),
        )

    for side, dx in enumerate((1, -1)):
        for array, layer, rows, to, lanes in tails(dx, True):
            tail_out[side, to, lanes] = array[layer, rows, last]

    def tail_copy(dx):
        side = (1, -1).index(dx)
        return pltpu.make_async_remote_copy(
            src_ref=tail_out.at[side], dst_ref=tail_in.at[side], send_sem=tail_send.at[side],
            recv_sem=tail_recv.at[side], device_id=(gx + dx, gy), device_id_type=MESH)

    def unpack(dx):
        side = (1, -1).index(dx)
        for array, layer, rows, to, lanes in tails(dx, False):
            array[layer, rows, last] = tail_in[side, to, lanes]

    pl.semaphore_wait(barrier, count - 1)

    for n in range(2):
        for dx, dy in DIRS:
            @pl.when(there(dx, dy))
            def _(n=n, dx=dx, dy=dy):
                halo(n, dx, dy).start()

    for dx in (1, -1):
        @pl.when(there(dx, 0))
        def _(dx=dx):
            tail_copy(dx).start()

    def arrived(directions):
        for n in range(2):
            for dx, dy in directions:
                @pl.when(there(-dx, -dy))
                def _(n=n, dx=dx, dy=dy):
                    halo(n, dx, dy).wait_recv()

    row = lax.broadcasted_iota(jnp.int32, (by + 2 * ROWS, bz), 0)
    inside_y = ((row >= ROWS) | (gy > 0)) & ((row < ROWS + by) | (gy < ny - 1))

    def inside(layer):
        ok = ((layer >= RIM) | (gx > 0)) & ((layer < RIM + bx) | (gx < nx - 1))
        return inside_y & ok

    inner = slice(ROWS, ROWS + by)

    def add_up(layer, span, f3, sums):
        k = layer - RIM
        rows = slice(span.start - ROWS, span.stop - ROWS)
        f0, f1, f2 = v0[layer, span], v1[layer, span], v2[layer, span]
        v1_ref[k, rows] = f1
        v2_ref[k, rows] = f2
        v3_ref[k, rows] = f3
        pairs = (f0 * f0, f0 * f1, f1 * f1, f1 * f2, f2 * f2, f2 * f3)
        groups = (span.stop - span.start) // 8
        return tuple(s + jnp.sum(p.reshape(groups, 8, bz), 0) for s, p in zip(sums, pairs))

    def body(layer, sums):
        return add_up(layer, inner, times_b(v2, dd, layer, None)[inner], sums)

    def stencils(starts, count, valid, sums):
        @pl.loop(0, count[0])
        def _(k):
            layer = starts[0] + k
            v1[layer] = times_b(v0, dd, layer, valid(layer))

        @pl.loop(0, count[1])
        def _(k):
            layer = starts[1] + k
            v2[layer] = times_b(v1, dd, layer, valid(layer))

        return lax.fori_loop(0, count[2], lambda k, s: body(starts[2] + k, s), sums)

    sums = (jnp.zeros((8, bz), jnp.float32),) * 6

    @pl.loop(RIM + 1, RIM + bx - 1)
    def _(layer):
        v1[layer, inner] = times_b(v0, dd, layer, None, inner)

    @pl.loop(RIM + 2, RIM + bx - 2)
    def _(layer):
        v2[layer, inner] = times_b(v1, dd, layer, None, inner)

    middle = slice(2 * ROWS, by)

    def middle_rows(layer, sums):
        f3 = times_b(v2, dd, layer, None, inner)[ROWS:by - ROWS]
        return add_up(layer, middle, f3, sums)

    sums = lax.fori_loop(RIM + 3, RIM + bx - 3, middle_rows, sums)

    arrived(DIRS[2:4])
    low_rows, high_rows = slice(0, 3 * ROWS), slice(by - ROWS, by + 2 * ROWS)
    low_in, high_in = gy > 0, gy < ny - 1
    short = lax.broadcasted_iota(jnp.int32, (3 * ROWS, bz), 0)
    low_ok = (short >= ROWS) | low_in
    high_ok = (short < 2 * ROWS) | high_in

    def ends(field, out, layer):
        out[layer, 0:2 * ROWS] = times_b(field, dd, layer, low_ok, low_rows)[:2 * ROWS]
        out[layer, by:by + 2 * ROWS] = times_b(field, dd, layer, high_ok, high_rows)[ROWS:]

    @pl.loop(RIM + 1, RIM + bx - 1)
    def _(layer):
        ends(v0, v1, layer)

    @pl.loop(RIM + 2, RIM + bx - 2)
    def _(layer):
        ends(v1, v2, layer)

    def end_rows(layer, sums):
        f3 = times_b(v2, dd, layer, None, low_rows)[ROWS:2 * ROWS]
        sums = add_up(layer, slice(ROWS, 2 * ROWS), f3, sums)
        f3 = times_b(v2, dd, layer, None, high_rows)[ROWS:2 * ROWS]
        return add_up(layer, slice(by, by + ROWS), f3, sums)

    sums = lax.fori_loop(RIM + 3, RIM + bx - 3, end_rows, sums)
    near_high = lax.rem(gx, 2) == 0
    for turn in range(2):
        high = near_high if turn == 0 else jnp.logical_not(near_high)

        @pl.when(high)
        def _():
            arrived([d for d in DIRS if d[0] < 0])

            @pl.when(there(1, 0))
            def _():
                tail_copy(-1).wait_recv()
                unpack(-1)

        @pl.when(jnp.logical_not(high))
        def _():
            arrived([d for d in DIRS if d[0] > 0])

            @pl.when(there(-1, 0))
            def _():
                tail_copy(1).wait_recv()
                unpack(1)

        starts = tuple(jnp.where(high, RIM + bx - 1 - k, RIM - 2 + k) for k in range(3))
        sums = stencils(starts, (3, 3, 3), inside, sums)

    lane = [jnp.sum(jnp.sum(s, 1, keepdims=True), 0, keepdims=True) for s in sums]
    lane_of = lax.broadcasted_iota(jnp.int32, (1, 128), 1)
    packed = jnp.zeros((1, 128), jnp.float32)
    for k, s in enumerate(lane):
        packed = jnp.where(lane_of == k, s, packed)
    part[0] = packed

    @pl.loop(1, count)
    def _(k):
        pltpu.make_async_remote_copy(
            src_ref=part.at[0], dst_ref=slots.at[me], send_sem=sum_send.at[0],
            recv_sem=sum_recv.at[0], device_id=peer(k), device_id_type=MESH).start()

    slots[me] = packed
    others = slots.at[pl.ds(0, count - 1)]
    pltpu.make_async_copy(others, others, sum_recv.at[0]).wait()
    total = jnp.sum(slots[...], 0)
    moments = [total[:, k:k + 1] for k in range(6)]
    row8 = lax.broadcasted_iota(jnp.int32, (8, 128), 0)
    co = jnp.zeros((8, 128), jnp.float32)
    for k, c in enumerate(coefficients(moments)):
        co = jnp.where(row8 == k, c, co)
    co_ref[...] = co
    pltpu.make_async_copy(others, others, sum_send.at[0]).wait()

    for n in range(2):
        for dx, dy in DIRS:
            @pl.when(there(dx, dy))
            def _(n=n, dx=dx, dy=dy):
                halo(n, dx, dy).wait_send()

    for dx in (1, -1):
        @pl.when(there(dx, 0))
        def _(dx=dx):
            tail_copy(dx).wait_send()


def combine(f0_ref, f1_ref, f2_ref, f3_ref, co_ref, x_ref, r_ref, x_out, r_out, sems):
    c = [co_ref[k:k + 1, 0:1] for k in range(7)]
    count = x_out.shape[0]

    def copy(n, k):
        src, dst = ((x_out, x_ref), (r_out, r_ref))[n]
        return pltpu.make_async_copy(src.at[pl.ds(k, 1)], dst.at[pl.ds(k, 1)], sems.at[n, k])

    @pl.loop(0, count)
    def _(k):
        f0, f1, f2, f3 = f0_ref[k], f1_ref[k], f2_ref[k], f3_ref[k]
        x_out[k] = c[0] * f0 + c[1] * f1 + c[2] * f2
        r_out[k] = c[3] * f0 + c[4] * f1 + c[5] * f2 + c[6] * f3
        for n in range(2):
            copy(n, k).start()

    @pl.loop(0, count)
    def _(k):
        for n in range(2):
            copy(n, k).wait()


def on_device(nx, ny, right_side, diagonal):
    bx, by, bz = right_side.shape
    block = jax.ShapeDtypeStruct((bx, by, bz), jnp.float32)
    big = pltpu.VMEM((bx + 2 * RIM, by + 2 * ROWS, bz), jnp.float32)
    vmem = pl.BlockSpec(memory_space=pltpu.VMEM)
    dma = pltpu.SemaphoreType.DMA
    f1, f2, f3, co = pl.pallas_call(
        functools.partial(kernel, nx, ny),
        out_shape=(block, block, block, jax.ShapeDtypeStruct((8, 128), jnp.float32)),
        in_specs=[pl.BlockSpec(memory_space=pltpu.HBM)] * 2,
        out_specs=(vmem,) * 4,
        scratch_shapes=[
            big, big, big, big,
            pltpu.VMEM((1, 1, 128), jnp.float32),
            pltpu.VMEM((nx * ny, 1, 128), jnp.float32),
            pltpu.VMEM((2, 2 * by + by // 2, 128), jnp.float32),
            pltpu.VMEM((2, 2 * by + by // 2, 128), jnp.float32),
            dma((2,)), dma((2, 8)), dma((2, 8)),
            dma((1,)), dma((1,)), dma((2,)), dma((2,)),
        ],
        compiler_params=pltpu.CompilerParams(
            collective_id=0, has_side_effects=True, vmem_limit_bytes=24 * 2**20),
    )(*(pltpu.with_memory_space_constraint(a, pltpu.HBM) for a in (right_side, diagonal)))
    return pl.pallas_call(
        combine,
        out_shape=(block, block),
        in_specs=[vmem] * 5,
        out_specs=(pl.BlockSpec(memory_space=pl.ANY),) * 2,
        scratch_shapes=[
            pltpu.VMEM((bx, by, bz), jnp.float32),
            pltpu.VMEM((bx, by, bz), jnp.float32),
            dma((2, bx)),
        ],
        compiler_params=pltpu.CompilerParams(vmem_limit_bytes=24 * 2**20),
    )(right_side, f1, f2, f3, co)


def solution(mesh):
    placed = (P("gx", "gy", None), P("gx", "gy", None))
    return jax.shard_map(
        functools.partial(on_device, mesh.shape["gx"], mesh.shape["gy"]),
        mesh=mesh,
        in_specs=placed,
        out_specs=placed,
        check_vma=False,
    )
```

```python
import functools

import jax
import jax.numpy as jnp
from jax import lax
from jax.experimental import pallas as pl
from jax.experimental.pallas import tpu as pltpu
from jax.sharding import PartitionSpec as P

ITERS = 3
SHIFT = 7.0
MESH = pl.DeviceIdType.MESH
DIRS = ((1, 0), (-1, 0), (0, 1), (0, -1), (1, 1), (1, -1), (-1, 1), (-1, -1))
RIM = ITERS
ROWS = 8


def span_x(step, width, size):
    if step == 0:
        return pl.ds(0, size), pl.ds(RIM, size)
    if step > 0:
        return pl.ds(size - width, width), pl.ds(RIM - width, width)
    return pl.ds(0, width), pl.ds(RIM + size, width)


def span_y(step, width, size):
    if step == 0:
        return pl.ds(0, size), pl.ds(ROWS, size)
    if step > 0:
        return pl.ds(size - width, width), pl.ds(ROWS - width, width)
    return pl.ds(0, width), pl.ds(ROWS + size, width)


def times_b(field, shift, layer, valid, span=slice(None)):
    here = field[layer, span]
    rows, lanes = here.shape
    row0 = jnp.zeros((1, lanes), jnp.float32)
    lane0 = jnp.zeros((rows, 1), jnp.float32)
    beside = field[layer - 1, span] + field[layer + 1, span]
    beside = beside + jnp.concatenate([here[1:], row0], 0)
    beside = beside + jnp.concatenate([row0, here[:-1]], 0)
    beside = beside + jnp.concatenate([here[:, 1:], lane0], 1)
    beside = beside + jnp.concatenate([lane0, here[:, :-1]], 1)
    out = (shift[layer, span] + (6.0 - SHIFT)) * here - beside
    if valid is None:
        return out
    return jnp.where(valid, out, 0.0)


def coefficients(moments):
    def inner(f, g):
        total = None
        for i, a in enumerate(f):
            for j, c in enumerate(g):
                term = a * c * moments[i + j]
                total = term if total is None else total + term
        return total

    def times_a(f):
        out = [SHIFT * f[0]]
        for k in range(1, len(f)):
            out.append(SHIFT * f[k] + f[k - 1])
        return out + [f[-1]]

    def axpy(f, a, g):
        size = max(len(f), len(g))
        out = []
        for k in range(size):
            if k >= len(f):
                out.append(a * g[k])
            elif k >= len(g):
                out.append(f[k])
            else:
                out.append(f[k] + a * g[k])
        return out

    one = jnp.ones_like(moments[0])
    residual, solution_field = [one], []
    s_field, p_field = [], []
    for step in range(ITERS):
        w_field = times_a(residual)
        gamma = inner(residual, residual)
        delta = inner(w_field, residual)
        if step == 0:
            alpha = gamma / delta
            s_field, p_field = w_field, residual
        else:
            beta = gamma / gamma_prev
            alpha = gamma / (delta - beta * gamma / alpha_prev)
            s_field = axpy(w_field, beta, s_field)
            p_field = axpy(residual, beta, p_field)
        solution_field = axpy(solution_field, alpha, p_field)
        residual = axpy(residual, -alpha, s_field)
        gamma_prev, alpha_prev = gamma, alpha
    return solution_field + residual


def kernel(nx, ny, b_ref, d_ref, v1_ref, v2_ref, v3_ref, co_ref,
           v0, dd, v1, v2, part, slots,
           tail_out, tail_in, own_sem, send_sem, recv_sem, sum_send, sum_recv, tail_send, tail_recv):
    gx, gy = lax.axis_index("gx"), lax.axis_index("gy")
    bx, by, bz = b_ref.shape
    barrier = pltpu.get_barrier_semaphore()

    def there(dx, dy):
        ok = None
        for at, step, count in ((gx, dx, nx), (gy, dy, ny)):
            if step:
                this = (at + step >= 0) & (at + step < count)
                ok = this if ok is None else ok & this
        return ok

    def peer_x(k):
        return lax.rem(gx + k, nx)

    def peer_y(k):
        return lax.rem(gy + k, ny)

    count = nx * ny
    me = gx * ny + gy

    def peer(k):
        to = lax.rem(me + k, count)
        return to // ny, lax.rem(to, ny)

    @pl.loop(1, count)
    def _(k):
        pl.semaphore_signal(barrier, inc=1, device_id=peer(k), device_id_type=MESH)

    own = []
    for n, (src, dst) in enumerate(((b_ref, v0), (d_ref, dd))):
        own.append(pltpu.make_async_copy(
            src, dst.at[pl.ds(RIM, bx), pl.ds(ROWS, by), :], own_sem.at[n]))
        own[-1].start()

    @pl.when(gx == 0)
    def _():
        v0[0:RIM] = jnp.zeros((RIM,) + v0.shape[1:], jnp.float32)

    @pl.when(gx == nx - 1)
    def _():
        v0[RIM + bx:] = jnp.zeros((RIM,) + v0.shape[1:], jnp.float32)

    @pl.when(gy == 0)
    def _():
        v0[:, 0:ROWS] = jnp.zeros((v0.shape[0], ROWS, bz), jnp.float32)

    @pl.when(gy == ny - 1)
    def _():
        v0[:, ROWS + by:] = jnp.zeros((v0.shape[0], ROWS, bz), jnp.float32)

    def halo(n, dx, dy):
        width = RIM - n if dx == 0 or dy == 0 else RIM - 1 - n
        width_y = width
        dst = (v0, dd)[n]
        src = dst.at[pl.ds(RIM, bx), pl.ds(ROWS, by), :]
        from_x, to_x = span_x(dx, width, bx)
        from_y, to_y = span_y(dy, width_y, by)
        index = DIRS.index((dx, dy))
        lanes = pl.ds(0, bz // 128 * 128) if dy == 0 else slice(None)
        return pltpu.make_async_remote_copy(
            src_ref=src.at[from_x, from_y, lanes],
            dst_ref=dst.at[to_x, to_y, lanes],
            send_sem=send_sem.at[n, index],
            recv_sem=recv_sem.at[n, index],
            device_id=(gx + dx, gy + dy),
            device_id_type=MESH,
        )

    for copy in own:
        copy.wait()
    full = bz // 128 * 128
    tail = bz - full
    half = by // 2
    last = pl.ds(full, tail)

    def tails(dx, sending):
        first, second = pl.ds(0, tail), pl.ds(tail, tail)
        low = {(True, 1): RIM + bx - 1, (True, -1): RIM, (False, 1): RIM - 1,
               (False, -1): RIM + bx}[sending, dx]
        at = [low - dx * k for k in range(RIM)]
        every = pl.ds(ROWS, by)
        return (
            (v0, at[0], every, pl.ds(0, by), first),
            (v0, at[1], every, pl.ds(0, by), second),
            (v0, at[2], every, pl.ds(by, by), first),
            (dd, at[0], every, pl.ds(by, by), second),
            (dd, at[1], pl.ds(ROWS, half), pl.ds(2 * by, half), first),
            (dd, at[1], pl.ds(ROWS + half, half), pl.ds(2 * by, half), second),
        )

    for side, dx in enumerate((1, -1)):
        for array, layer, rows, to, lanes in tails(dx, True):
            tail_out[side, to, lanes] = array[layer, rows, last]

    def tail_copy(dx):
        side = (1, -1).index(dx)
        return pltpu.make_async_remote_copy(
            src_ref=tail_out.at[side], dst_ref=tail_in.at[side], send_sem=tail_send.at[side],
            recv_sem=tail_recv.at[side], device_id=(gx + dx, gy), device_id_type=MESH)

    def unpack(dx):
        side = (1, -1).index(dx)
        for array, layer, rows, to, lanes in tails(dx, False):
            array[layer, rows, last] = tail_in[side, to, lanes]

    pl.semaphore_wait(barrier, count - 1)

    for n in range(2):
        for dx, dy in DIRS:
            @pl.when(there(dx, dy))
            def _(n=n, dx=dx, dy=dy):
                halo(n, dx, dy).start()

    for dx in (1, -1):
        @pl.when(there(dx, 0))
        def _(dx=dx):
            tail_copy(dx).start()

    def arrived(directions):
        for n in range(2):
            for dx, dy in directions:
                @pl.when(there(-dx, -dy))
                def _(n=n, dx=dx, dy=dy):
                    halo(n, dx, dy).wait_recv()

    row = lax.broadcasted_iota(jnp.int32, (by + 2 * ROWS, bz), 0)
    inside_y = ((row >= ROWS) | (gy > 0)) & ((row < ROWS + by) | (gy < ny - 1))

    def inside(layer):
        ok = ((layer >= RIM) | (gx > 0)) & ((layer < RIM + bx) | (gx < nx - 1))
        return inside_y & ok

    inner = slice(ROWS, ROWS + by)

    def add_up(layer, span, f3, sums):
        k = layer - RIM
        rows = slice(span.start - ROWS, span.stop - ROWS)
        f0, f1, f2 = v0[layer, span], v1[layer, span], v2[layer, span]
        v1_ref[k, rows] = f1
        v2_ref[k, rows] = f2
        v3_ref[k, rows] = f3
        pairs = (f0 * f0, f0 * f1, f1 * f1, f1 * f2, f2 * f2, f2 * f3)
        groups = (span.stop - span.start) // 8
        return tuple(s + jnp.sum(p.reshape(groups, 8, bz), 0) for s, p in zip(sums, pairs))

    def body(layer, sums):
        return add_up(layer, inner, times_b(v2, dd, layer, None)[inner], sums)

    def stencils(starts, count, valid, sums):
        @pl.loop(0, count[0], unroll=True)
        def _(k):
            layer = starts[0] + k
            v1[layer] = times_b(v0, dd, layer, valid(layer))

        @pl.loop(0, count[1], unroll=True)
        def _(k):
            layer = starts[1] + k
            v2[layer] = times_b(v1, dd, layer, valid(layer))

        return lax.fori_loop(0, count[2], lambda k, s: body(starts[2] + k, s), sums, unroll=True)

    sums = (jnp.zeros((8, bz), jnp.float32),) * 6

    @pl.loop(RIM + 1, RIM + bx - 1, unroll=2)
    def _(layer):
        v1[layer, inner] = times_b(v0, dd, layer, None, inner)

    @pl.loop(RIM + 2, RIM + bx - 2, unroll=2)
    def _(layer):
        v2[layer, inner] = times_b(v1, dd, layer, None, inner)

    middle = slice(2 * ROWS, by)

    def middle_rows(layer, sums):
        f3 = times_b(v2, dd, layer, None, inner)[ROWS:by - ROWS]
        return add_up(layer, middle, f3, sums)

    sums = lax.fori_loop(RIM + 3, RIM + bx - 3, middle_rows, sums, unroll=2)

    arrived(DIRS[2:4])
    low_rows, high_rows = slice(0, 3 * ROWS), slice(by - ROWS, by + 2 * ROWS)
    low_in, high_in = gy > 0, gy < ny - 1
    short = lax.broadcasted_iota(jnp.int32, (3 * ROWS, bz), 0)
    low_ok = (short >= ROWS) | low_in
    high_ok = (short < 2 * ROWS) | high_in

    def ends(field, out, layer):
        out[layer, 0:2 * ROWS] = times_b(field, dd, layer, low_ok, low_rows)[:2 * ROWS]
        out[layer, by:by + 2 * ROWS] = times_b(field, dd, layer, high_ok, high_rows)[ROWS:]

    @pl.loop(RIM + 1, RIM + bx - 1, unroll=2)
    def _(layer):
        ends(v0, v1, layer)

    @pl.loop(RIM + 2, RIM + bx - 2, unroll=2)
    def _(layer):
        ends(v1, v2, layer)

    def end_rows(layer, sums):
        f3 = times_b(v2, dd, layer, None, low_rows)[ROWS:2 * ROWS]
        sums = add_up(layer, slice(ROWS, 2 * ROWS), f3, sums)
        f3 = times_b(v2, dd, layer, None, high_rows)[ROWS:2 * ROWS]
        return add_up(layer, slice(by, by + ROWS), f3, sums)

    sums = lax.fori_loop(RIM + 3, RIM + bx - 3, end_rows, sums, unroll=2)
    near_high = lax.rem(gx, 2) == 0
    for turn in range(2):
        high = near_high if turn == 0 else jnp.logical_not(near_high)

        @pl.when(high)
        def _():
            arrived([d for d in DIRS if d[0] < 0])

            @pl.when(there(1, 0))
            def _():
                tail_copy(-1).wait_recv()
                unpack(-1)

        @pl.when(jnp.logical_not(high))
        def _():
            arrived([d for d in DIRS if d[0] > 0])

            @pl.when(there(-1, 0))
            def _():
                tail_copy(1).wait_recv()
                unpack(1)

        starts = tuple(jnp.where(high, RIM + bx - 1 - k, RIM - 2 + k) for k in range(3))
        sums = stencils(starts, (3, 3, 3), inside, sums)

    lane = [jnp.sum(jnp.sum(s, 1, keepdims=True), 0, keepdims=True) for s in sums]
    lane_of = lax.broadcasted_iota(jnp.int32, (1, 128), 1)
    packed = jnp.zeros((1, 128), jnp.float32)
    for k, s in enumerate(lane):
        packed = jnp.where(lane_of == k, s, packed)
    part[0] = packed

    @pl.loop(1, count)
    def _(k):
        pltpu.make_async_remote_copy(
            src_ref=part.at[0], dst_ref=slots.at[me], send_sem=sum_send.at[0],
            recv_sem=sum_recv.at[0], device_id=peer(k), device_id_type=MESH).start()

    slots[me] = packed
    others = slots.at[pl.ds(0, count - 1)]
    pltpu.make_async_copy(others, others, sum_recv.at[0]).wait()
    total = jnp.sum(slots[...], 0)
    moments = [total[:, k:k + 1] for k in range(6)]
    row8 = lax.broadcasted_iota(jnp.int32, (8, 128), 0)
    co = jnp.zeros((8, 128), jnp.float32)
    for k, c in enumerate(coefficients(moments)):
        co = jnp.where(row8 == k, c, co)
    co_ref[...] = co
    pltpu.make_async_copy(others, others, sum_send.at[0]).wait()

    for n in range(2):
        for dx, dy in DIRS:
            @pl.when(there(dx, dy))
            def _(n=n, dx=dx, dy=dy):
                halo(n, dx, dy).wait_send()

    for dx in (1, -1):
        @pl.when(there(dx, 0))
        def _(dx=dx):
            tail_copy(dx).wait_send()


def combine(f0_ref, f1_ref, f2_ref, f3_ref, co_ref, x_ref, r_ref, x_out, r_out, sems):
    c = [co_ref[k:k + 1, 0:1] for k in range(7)]
    count = x_out.shape[0]

    def copy(n, k):
        src, dst = ((x_out, x_ref), (r_out, r_ref))[n]
        return pltpu.make_async_copy(src.at[pl.ds(k, 1)], dst.at[pl.ds(k, 1)], sems.at[n, k])

    @pl.loop(0, count)
    def _(k):
        f0, f1, f2, f3 = f0_ref[k], f1_ref[k], f2_ref[k], f3_ref[k]
        x_out[k] = c[0] * f0 + c[1] * f1 + c[2] * f2
        r_out[k] = c[3] * f0 + c[4] * f1 + c[5] * f2 + c[6] * f3
        for n in range(2):
            copy(n, k).start()

    @pl.loop(0, count)
    def _(k):
        for n in range(2):
            copy(n, k).wait()


def on_device(nx, ny, right_side, diagonal):
    bx, by, bz = right_side.shape
    block = jax.ShapeDtypeStruct((bx, by, bz), jnp.float32)
    big = pltpu.VMEM((bx + 2 * RIM, by + 2 * ROWS, bz), jnp.float32)
    vmem = pl.BlockSpec(memory_space=pltpu.VMEM)
    dma = pltpu.SemaphoreType.DMA
    f1, f2, f3, co = pl.pallas_call(
        functools.partial(kernel, nx, ny),
        out_shape=(block, block, block, jax.ShapeDtypeStruct((8, 128), jnp.float32)),
        in_specs=[pl.BlockSpec(memory_space=pltpu.HBM)] * 2,
        out_specs=(vmem,) * 4,
        scratch_shapes=[
            big, big, big, big,
            pltpu.VMEM((1, 1, 128), jnp.float32),
            pltpu.VMEM((nx * ny, 1, 128), jnp.float32),
            pltpu.VMEM((2, 2 * by + by // 2, 128), jnp.float32),
            pltpu.VMEM((2, 2 * by + by // 2, 128), jnp.float32),
            dma((2,)), dma((2, 8)), dma((2, 8)),
            dma((1,)), dma((1,)), dma((2,)), dma((2,)),
        ],
        compiler_params=pltpu.CompilerParams(
            collective_id=0, has_side_effects=True, vmem_limit_bytes=24 * 2**20),
    )(*(pltpu.with_memory_space_constraint(a, pltpu.HBM) for a in (right_side, diagonal)))
    return pl.pallas_call(
        combine,
        out_shape=(block, block),
        in_specs=[vmem] * 5,
        out_specs=(pl.BlockSpec(memory_space=pl.ANY),) * 2,
        scratch_shapes=[
            pltpu.VMEM((bx, by, bz), jnp.float32),
            pltpu.VMEM((bx, by, bz), jnp.float32),
            dma((2, bx)),
        ],
        compiler_params=pltpu.CompilerParams(vmem_limit_bytes=24 * 2**20),
    )(right_side, f1, f2, f3, co)


def solution(mesh):
    placed = (P("gx", "gy", None), P("gx", "gy", None))
    return jax.shard_map(
        functools.partial(on_device, mesh.shape["gx"], mesh.shape["gy"]),
        mesh=mesh,
        in_specs=placed,
        out_specs=placed,
        check_vma=False,
    )
```
